16 devices in a mesh: col: 2 (over z), row: 8 (over y, x, core).
Axes of the slice: x: 2, y: 2, z: 2, core: 2. Of those that a mesh axis runs over, the one named last changes fastest.
Arguments:
- x_in: bfloat16 [16384, 2048], P('row', 'col')
- ln_gain: float32 [2048], P('col')
- ln_bias: float32 [2048], P('col')
- w_up: bfloat16 [2048, 8192], P('row', 'col')
- b_up: bfloat16 [8192], P('col')
- w_down: bfloat16 [8192, 2048], P('row', 'col')
- b_down: bfloat16 [2048], P('col')
- dy_out: bfloat16 [16384, 2048], P('row', 'col')
Outputs:
- output 1: bfloat16 [16384, 2048], P('row', 'col')
- output 2: bfloat16 [16384, 2048], P('row', 'col')
- output 3: bfloat16 [2048, 8192], P('row', 'col')
- output 4: float32 [8192], P('col')
- output 5: bfloat16 [8192, 2048], P('row', 'col')
- output 6: float32 [2048], P('col')
- output 7: float32 [2048], P('col')
- output 8: float32 [2048], P('col')
All inputs are finite; a program needn't handle non-finite values.
Results may differ from the reference program's by a relative error of at most 0.0112856.
Values are sent between devices in bfloat16 or wider.
A program may use at most 1 GiB of HBM per device.

```python
import jax
import jax.numpy as jnp
from jax import lax

TOKENS = 16384
D = 2048
FF = 8192
LN_EPS = 1e-5
GELU_K = 0.7978845608028654
GELU_A = 0.044715


def setup_inputs(seed: int = 0) -> dict:
    keys = jax.random.split(jax.random.key(seed), 12)
    col_mean = jax.random.normal(keys[0], (1, D), jnp.float32)
    col_scale = 0.5 + jax.random.uniform(keys[1], (1, D), jnp.float32)
    row_shift = 0.5 * jax.random.normal(keys[2], (TOKENS, 1), jnp.float32)
    x_base = jax.random.normal(keys[3], (TOKENS, D), jnp.float32)
    x_in = (x_base * col_scale + col_mean + row_shift).astype(jnp.bfloat16)
    ln_gain = 0.5 + jax.random.uniform(keys[4], (D,), jnp.float32)
    ln_bias = 0.3 * jax.random.normal(keys[5], (D,), jnp.float32)
    w_up = (jax.random.normal(keys[6], (D, FF), jnp.float32) * D ** -0.5).astype(jnp.bfloat16)
    b_up = (0.5 * jax.random.normal(keys[7], (FF,), jnp.float32)).astype(jnp.bfloat16)
    w_down = (jax.random.normal(keys[8], (FF, D), jnp.float32) * (1.5 * FF ** -0.5)).astype(jnp.bfloat16)
    b_down = (0.5 * jax.random.normal(keys[9], (D,), jnp.float32)).astype(jnp.bfloat16)
    dy_out = jax.random.normal(keys[10], (TOKENS, D), jnp.float32).astype(jnp.bfloat16)
    return {'x_in': x_in, 'ln_gain': ln_gain, 'ln_bias': ln_bias, 'w_up': w_up, 'b_up': b_up, 'w_down': w_down, 'b_down': b_down, 'dy_out': dy_out}


def gelu_grad(u_val):
    tanh_val = jnp.tanh(GELU_K * (u_val + GELU_A * u_val * u_val * u_val))
    slope = GELU_K * (1.0 + 3.0 * GELU_A * u_val * u_val)
    return 0.5 * (1.0 + tanh_val) + 0.5 * u_val * (1.0 - tanh_val * tanh_val) * slope


def reference(x_in, ln_gain, ln_bias, w_up, b_up, w_down, b_down, dy_out):
    width = x_in.shape[1]
    x_f32 = x_in.astype(jnp.float32)
    mean_x = jnp.sum(x_f32, axis=1, keepdims=True) / width
    mean_sq = jnp.sum(x_f32 * x_f32, axis=1, keepdims=True) / width
    inv_std = lax.rsqrt(mean_sq - mean_x * mean_x + LN_EPS)
    x_hat = (x_f32 - mean_x) * inv_std
    z_act = (x_hat * ln_gain + ln_bias).astype(jnp.bfloat16)
    u_pre = (jnp.dot(z_act, w_up, preferred_element_type=jnp.float32) + b_up.astype(jnp.float32)).astype(jnp.bfloat16)
    u_f32 = u_pre.astype(jnp.float32)
    a_act = jax.nn.gelu(u_f32, approximate=True).astype(jnp.bfloat16)
    y_out = (x_f32 + jnp.dot(a_act, w_down, preferred_element_type=jnp.float32) + b_down.astype(jnp.float32)).astype(jnp.bfloat16)
    dy_f32 = dy_out.astype(jnp.float32)
    d_act = jnp.dot(dy_out, w_down.T, preferred_element_type=jnp.float32)
    du_pre = (d_act * gelu_grad(u_f32)).astype(jnp.bfloat16)
    dw_down = jnp.dot(a_act.T, dy_out, preferred_element_type=jnp.float32).astype(jnp.bfloat16)
    db_down = jnp.sum(dy_f32, axis=0)
    dw_up = jnp.dot(z_act.T, du_pre, preferred_element_type=jnp.float32).astype(jnp.bfloat16)
    db_up = jnp.sum(du_pre.astype(jnp.float32), axis=0)
    dz_act = jnp.dot(du_pre, w_up.T, preferred_element_type=jnp.float32)
    d_gain = jnp.sum(dz_act * x_hat, axis=0)
    d_bias = jnp.sum(dz_act, axis=0)
    d_xhat = dz_act * ln_gain
    mean_dxh = jnp.sum(d_xhat, axis=1, keepdims=True) / width
    mean_dxh_xh = jnp.sum(d_xhat * x_hat, axis=1, keepdims=True) / width
    dx_in = (dy_f32 + inv_std * (d_xhat - mean_dxh - x_hat * mean_dxh_xh)).astype(jnp.bfloat16)
    return (y_out, dx_in, dw_up, db_up, dw_down, db_down, d_gain, d_bias)
```

```python
import jax
import jax.numpy as jnp
from jax import lax
from jax.sharding import PartitionSpec as P

LN_EPS = 1e-5
GELU_K = 0.7978845608028654
GELU_A = 0.044715
CONTRACT_ROWS = (((0,), (0,)), ((), ()))
CONTRACT_COLS = (((1,), (1,)), ((), ()))
CHUNKS = 4
BF16 = jnp.bfloat16
F32 = jnp.float32


def gelu_grad(u_val):
    tanh_val = jnp.tanh(GELU_K * (u_val + GELU_A * u_val * u_val * u_val))
    slope = GELU_K * (1.0 + 3.0 * GELU_A * u_val * u_val)
    return 0.5 * (1.0 + tanh_val) + 0.5 * u_val * (1.0 - tanh_val * tanh_val) * slope


def dot(a, b, dims=None):
    if dims is None:
        return jnp.dot(a, b, preferred_element_type=F32)
    return lax.dot_general(a, b, dims, preferred_element_type=F32)


def spread_perm(flip):
    pairs = []
    for y in range(2):
        for x in range(2):
            for c in range(2):
                for z in range(2):
                    src = ((z * 2 + y) * 2 + x) * 2 + c
                    dst = ((y * 2 + x) * 2 + c) * 2 + (z ^ flip)
                    pairs.append((src, dst))
    return pairs


def invert(pairs):
    return [(d, s) for s, d in pairs]


def solution(mesh):
    perm_a, perm_b = spread_perm(0), spread_perm(1)

    def local_step(x_in, ln_gain, ln_bias, w_up, b_up, w_down, b_down, dy_out):
        col = lax.axis_index('col')
        core = lax.rem(lax.axis_index('row'), 2)
        tokens, half = x_in.shape
        width = half * 2
        first = col == 0
        straight = core == col

        def swap(v):
            return lax.ppermute(v, 'col', [(0, 1), (1, 0)])

        w_up_all = lax.all_gather(w_up, 'row', axis=0, tiled=True)
        rows = w_down.shape[0] // 2
        send_a = lax.dynamic_slice_in_dim(w_down, col * rows, rows, 0)
        send_b = lax.dynamic_slice_in_dim(w_down, (1 - col) * rows, rows, 0)
        got_a = lax.ppermute(send_a, ('col', 'row'), perm_a)
        got_b = lax.ppermute(send_b, ('col', 'row'), perm_b)
        piece = jnp.concatenate([jnp.where(straight, got_a, got_b), jnp.where(straight, got_b, got_a)], axis=1)
        w_dn = lax.all_gather(piece, 'row', axis=0, tiled=True)

        x_oth = swap(x_in)
        ln_vec = jnp.stack([ln_gain, ln_bias])
        ln_vec_oth = swap(ln_vec)
        dy_oth = swap(dy_out)

        x_f32 = x_in.astype(F32)
        xo_f32 = x_oth.astype(F32)
        mean_x = (jnp.sum(x_f32, axis=1, keepdims=True) + jnp.sum(xo_f32, axis=1, keepdims=True)) / width
        mean_sq = (jnp.sum(x_f32 * x_f32, axis=1, keepdims=True) + jnp.sum(xo_f32 * xo_f32, axis=1, keepdims=True)) / width
        inv_std = lax.rsqrt(mean_sq - mean_x * mean_x + LN_EPS)
        x_hat = (x_f32 - mean_x) * inv_std
        left = jnp.where(first, x_in, x_oth).astype(F32)
        right = jnp.where(first, x_oth, x_in).astype(F32)
        vec_l = jnp.where(first, ln_vec, ln_vec_oth)
        vec_r = jnp.where(first, ln_vec_oth, ln_vec)
        z_act = jnp.concatenate([
            ((left - mean_x) * inv_std * vec_l[0] + vec_l[1]).astype(BF16),
            ((right - mean_x) * inv_std * vec_r[0] + vec_r[1]).astype(BF16)], axis=1)
        u_pre = (dot(z_act, w_up_all) + b_up.astype(F32)).astype(BF16)
        u_f32 = u_pre.astype(F32)
        a_act = jax.nn.gelu(u_f32, approximate=True).astype(BF16)

        m = tokens // CHUNKS
        dy_f32 = dy_out.astype(F32)
        y_parts = []
        for k in range(CHUNKS):
            a_k = a_act[k * m:(k + 1) * m]
            y_send = swap(dot(a_k, w_dn[:, half:]))
            y_keep = dot(a_k, w_dn[:, :half])
            y_parts.append((x_f32[k * m:(k + 1) * m] + (y_keep + y_send) + b_down.astype(F32)).astype(BF16))
        y_out = jnp.concatenate(y_parts, axis=0)

        dy_cat = jnp.concatenate([dy_out, dy_oth], axis=1)
        dwd_part = dot(a_act, dy_cat, CONTRACT_ROWS)
        dwd = lax.psum_scatter(dwd_part, 'row', scatter_dimension=0, tiled=True).astype(BF16)
        d_own, d_oth = dwd[:, :half], dwd[:, half:]
        back_a = lax.ppermute(jnp.where(straight, d_own, d_oth), ('col', 'row'), invert(perm_a))
        back_b = lax.ppermute(jnp.where(straight, d_oth, d_own), ('col', 'row'), invert(perm_b))
        dw_down = jnp.concatenate([jnp.where(first, back_a, back_b), jnp.where(first, back_b, back_a)], axis=0)
        db_down = jnp.sum(dy_f32, axis=0)

        d_act = dot(dy_cat, w_dn, CONTRACT_COLS)
        du_pre = (d_act * gelu_grad(u_f32)).astype(BF16)
        db_up = jnp.sum(du_pre.astype(F32), axis=0)

        w_own = lax.dynamic_slice_in_dim(w_up_all, col * half, half, 0)
        w_oth = lax.dynamic_slice_in_dim(w_up_all, (1 - col) * half, half, 0)
        dx_parts = []
        sums = jnp.zeros((2, half), F32)
        for k in range(CHUNKS):
            sl = slice(k * m, (k + 1) * m)
            du_k = du_pre[sl]
            got = swap(dot(du_k, w_oth, CONTRACT_COLS))
            dz = dot(du_k, w_own, CONTRACT_COLS) + got
            xh = x_hat[sl]
            sums = sums + jnp.stack([jnp.sum(dz * xh, axis=0), jnp.sum(dz, axis=0)])
            e = dz * ln_gain
            rs = jnp.stack([jnp.sum(e, axis=1), jnp.sum(e * xh, axis=1)])
            rs = (rs + swap(rs)) / width
            dx_parts.append((dy_f32[sl] + inv_std[sl] * (e - rs[0][:, None] - xh * rs[1][:, None])).astype(BF16))
        dx_in = jnp.concatenate(dx_parts, axis=0)

        dwu_part = dot(z_act, du_pre, CONTRACT_ROWS)
        dw_up = lax.psum_scatter(dwu_part, 'row', scatter_dimension=0, tiled=True).astype(BF16)

        db_up, db_down, sums = lax.psum((db_up, db_down, sums), 'row')
        return (y_out, dx_in, dw_up, db_up, dw_down, db_down, sums[0], sums[1])

    blk_spec = P('row', 'col')
    vec_spec = P('col')
    return jax.shard_map(local_step, mesh=mesh, in_specs=(blk_spec, vec_spec, vec_spec, blk_spec, vec_spec, blk_spec, vec_spec, blk_spec), out_specs=(blk_spec, blk_spec, blk_spec, vec_spec, blk_spec, vec_spec, vec_spec, vec_spec), check_vma=False)
```
